32 devices in a mesh: leaf: 8 (over y, x, core), rows: 4 (over z).
Axes of the slice: x: 2, y: 2, z: 4, core: 2. Of those that a mesh axis runs over, the one named last changes fastest.
Arguments:
- right_side: float32 [8, 2, 64, 512], P('leaf', None, None, 'rows'), as said below
- diag_inverse: float32 [8, 2, 512, 128], P('leaf', None, 'rows'), as said below
- sep_lower: float32 [8, 2, 512, 512], P('leaf', None, 'rows'), as said below
- front_lower: float32 [8, 2, 1024, 512], P('leaf', None, None, 'rows'), as said below
- front_index: int32 [8, 2, 1024], P('leaf'), may hold values from 0 to 1535, as said below
Outputs:
- solution: float32 [8, 2, 64, 512], P('leaf', None, None, 'rows')
- top_update: float32 [8, 2, 64, 512], P('leaf', None, None, 'rows')
The draws below stay inside these ranges and needn't reach their ends.
Inputs may be any that keep to these rules, and one draw needn't show every extreme that they name: `front_index`: for each leaf index and slot s the 1024 entries are distinct, lie below (3 - s) * 512, and are the same on all 2**s leaf indices of the slot's subtree. `right_side`: entries of slot s are the same on all 2**s leaf indices of the slot's subtree. `diag_inverse`: entries of slot s are the same on all 2**s leaf indices of the slot's subtree. `sep_lower`: entries of slot s are the same on all 2**s leaf indices of the slot's subtree. `front_lower`: entries of slot s are the same on all 2**s leaf indices of the slot's subtree.
All inputs are finite; a program needn't handle non-finite values.
Results may differ from the reference program's by a relative error of at most 0.00011.
Values sent between devices are 32-bit elements; how exact they have to be, the bound alone decides.
A program may use at most 128 MiB of HBM per device.

```python
from functools import partial
import jax
import jax.numpy as jnp
from jax import lax

NVEC = 64
BLK = 128
FR = 1024
LEAVES = 8
DEPTH = 3
LEVELS = 2
SEP = 512
N_ROWS = 4


def node_blocks(key, tail, maker):
    stacked = []
    for level in range(LEVELS):
        count = LEAVES // 2 ** level
        values = maker(jax.random.fold_in(key, level), (count,) + tail)
        stacked.append(jnp.repeat(values, 2 ** level, axis=0))
    return jnp.stack(stacked, axis=1)


def right_maker(subkey, shape):
    return jnp.clip(jax.random.normal(subkey, shape, jnp.float32), -5.0, 5.0)


def draw_right_side(key, part):
    return node_blocks(key, (NVEC, SEP), right_maker)


def inverse_maker(subkey, shape):
    identity = jnp.tile(jnp.eye(BLK, dtype=jnp.float32), (SEP // BLK, 1))
    return identity + 0.4 / BLK ** 0.5 * jax.random.normal(subkey, shape, jnp.float32)


def draw_diag_inverse(key, part):
    return node_blocks(key, (SEP, BLK), inverse_maker)


def lower_maker(subkey, shape):
    return jax.random.normal(subkey, shape, jnp.float32) / SEP ** 0.5


def draw_sep_lower(key, part):
    return node_blocks(key, (SEP, SEP), lower_maker)


def front_maker(subkey, shape):
    return 0.5 * jax.random.normal(subkey, shape, jnp.float32) / SEP ** 0.5


def draw_front_lower(key, part):
    return node_blocks(key, (FR, SEP), front_maker)


def draw_front_index(key, part):
    total_width = DEPTH * SEP
    stacked = []
    for level in range(LEVELS):
        count = LEAVES // 2 ** level
        reach = (DEPTH - level) * SEP
        scores = jax.random.randint(jax.random.fold_in(key, level), (count, total_width), 0, 262144, dtype=jnp.int32)
        places = jnp.arange(total_width, dtype=jnp.int32)
        keyed = jnp.where(places[None, :] < reach, scores * total_width + places[None, :], -1)
        chosen = lax.top_k(keyed, FR)[1].astype(jnp.int32)
        stacked.append(jnp.repeat(chosen, 2 ** level, axis=0))
    return jnp.stack(stacked, axis=1)


def setup_inputs(seed: int = 0) -> dict:
    key_list = jax.random.split(jax.random.key(seed), 6)
    right_side = draw_right_side(jax.random.fold_in(key_list[5], 71), 0)
    diag_inverse = draw_diag_inverse(jax.random.fold_in(key_list[5], 71), 0)
    sep_lower = draw_sep_lower(jax.random.fold_in(key_list[5], 71), 0)
    front_lower = draw_front_lower(jax.random.fold_in(key_list[5], 71), 0)
    front_index = draw_front_index(jax.random.fold_in(key_list[5], 71), 0)
    return dict(right_side=right_side, diag_inverse=diag_inverse, sep_lower=sep_lower, front_lower=front_lower, front_index=front_index)


exact_precision = lax.Precision.HIGHEST


def product(left, right):
    return lax.dot_general(left, right, (((left.ndim - 1,), (right.ndim - 1,)), ((), ())), precision=exact_precision, preferred_element_type=jnp.float32)


def solve_rows(target, inverse, prefixes, width):
    solved = []
    for block, prefix in enumerate(prefixes):
        first = block * width
        total = target[:, first:first + width]
        if block > 0:
            total = total - product(jnp.concatenate(solved, axis=1), prefix)
        solved.append(product(total, inverse[first:first + width]))
    return jnp.concatenate(solved, axis=1)


def solve_separator(target, inverse, lower, blocks, width):
    prefixes = [lower[block * width:(block + 1) * width, :block * width] for block in range(blocks)]
    return solve_rows(target, inverse, prefixes, width)


def add_columns(held, columns, added):
    return held.at[:, columns].add(added)


def reference(right_side, diag_inverse, sep_lower, front_lower, front_index):
    pending = jnp.zeros((LEAVES, NVEC, DEPTH * SEP), jnp.float32)
    solutions = []
    solver = jax.vmap(partial(solve_separator, blocks=N_ROWS, width=BLK))
    for level in range(LEVELS):
        height = DEPTH - level
        if level > 0:
            group = 2 ** (level - 1)
            paired = pending.reshape(LEAVES // (2 * group), 2, group, NVEC, pending.shape[2])
            paired = jnp.broadcast_to(jnp.sum(paired, axis=1, keepdims=True), paired.shape)
            pending = paired.reshape(LEAVES, NVEC, paired.shape[4])
            target = right_side[:, level] - pending[:, :, height * SEP:(height + 1) * SEP]
        else:
            target = right_side[:, 0]
        pending = pending[:, :, :height * SEP]
        solved = solver(target, diag_inverse[:, level], sep_lower[:, level])
        solutions.append(solved)
        frontal = jax.vmap(product)(solved, front_lower[:, level])
        pending = jax.vmap(add_columns)(pending, front_index[:, level], frontal)
    top = pending.reshape(LEAVES, NVEC, 2, SEP).transpose(0, 2, 1, 3)
    return jnp.stack(solutions, axis=1), top
```

```python
import functools

import jax
import jax.numpy as jnp
from jax import lax
from jax.experimental import pallas as pl
from jax.experimental.pallas import tpu as pltpu
from jax.sharding import PartitionSpec as P

MESH = pl.DeviceIdType.MESH
F32 = jnp.float32
BF16 = jnp.bfloat16


def split(value):
    high = value.astype(BF16)
    low = (value - high.astype(F32)).astype(BF16)
    return high, low


def dot_nt(left, right):
    return lax.dot_general(
        left, right, (((1,), (1,)), ((), ())), preferred_element_type=F32
    )


def product(left, right):
    return (
        dot_nt(left[0], right[1]) + dot_nt(left[1], right[0])
    ) + dot_nt(left[0], right[0])


def kernel(
    blocks,
    rs_ref,
    idx_ref,
    diag_hbm,
    lower_hbm,
    front_hbm,
    sol_ref,
    top_ref,
    ld0,
    ld1,
    front,
    place_t,
    place_u,
    spread,
    gather_f,
    xs,
    part_t,
    part_u,
    recv_t,
    recv_u,
    ag,
    own_half,
    other_half,
    load_sem,
    x_sem,
    ld_sem,
    lf_sem,
    g_sem,
    gf_sem,
    t_sem,
    u_sem,
    ag_sem,
    out_sem,
):
    vectors, width = rs_ref.shape[2], rs_ref.shape[3]
    half = vectors // 2
    sep = blocks * width
    rows_half = width // 2
    leaf = lax.axis_index("leaf")
    me = lax.axis_index("rows")
    core = lax.rem(leaf, 2)
    first_leaf = leaf - core
    partner = (leaf + 1 - 2 * core, me)

    def remote(src, dst, sems, out_slot, in_slot, device):
        return pltpu.make_async_remote_copy(
            src_ref=src,
            dst_ref=dst,
            send_sem=sems.at[0, out_slot],
            recv_sem=sems.at[1, in_slot],
            device_id=device,
            device_id_type=MESH,
        )

    loads = [
        pltpu.make_async_copy(diag_hbm.at[0, 0], ld0.at[:, pl.ds(0, width)], load_sem.at[0]),
        pltpu.make_async_copy(lower_hbm.at[0, 0], ld0.at[:, pl.ds(width, sep)], load_sem.at[1]),
        pltpu.make_async_copy(diag_hbm.at[0, 1], ld1.at[me, :, pl.ds(0, width)], load_sem.at[2]),
        pltpu.make_async_copy(lower_hbm.at[0, 1], ld1.at[me, :, pl.ds(width, sep)], load_sem.at[3]),
        pltpu.make_async_copy(front_hbm.at[0, 0], front.at[0], load_sem.at[4]),
        pltpu.make_async_copy(front_hbm.at[0, 1], front.at[1], load_sem.at[5]),
    ]
    for load in loads:
        load.start()

    barrier = pltpu.get_barrier_semaphore()
    pl.semaphore_signal(barrier, inc=1, device_id=partner, device_id_type=MESH)
    for q in range(blocks):
        @pl.when(q != me)
        def _():
            for c in range(2):
                pl.semaphore_signal(
                    barrier, inc=1, device_id=(first_leaf + c, q), device_id_type=MESH
                )

    def x_copy(q):
        return remote(xs.at[me], xs.at[me], x_sem, q, me, (leaf, q))

    def x_arrival(e):
        return remote(xs.at[e], xs.at[e], x_sem, e, e, (leaf, e))

    def finish_x(total):
        x = product(split(total), split(ld0[:, :width]))
        xs[me] = x
        for q in range(1, blocks):
            @pl.when(q > me)
            def _():
                x_copy(q).start()

    loads[0].wait()
    loads[1].wait()
    pl.semaphore_wait(barrier, 2 * blocks - 1)

    @pl.when(me == 0)
    def _():
        finish_x(rs_ref[0, 0])

    loads[2].wait()
    loads[3].wait()

    def ld_rows(r, c):
        return ld1.at[
            r,
            pl.ds(pl.multiple_of(c * rows_half, rows_half), rows_half),
            pl.ds(0, (r + 1) * width),
        ]

    def ld_own_rows(r):
        return ld1.at[
            me,
            pl.ds(pl.multiple_of(core * rows_half, rows_half), rows_half),
            pl.ds(0, (r + 1) * width),
        ]

    for r in range(blocks):
        @pl.when(me == r)
        def _():
            for q in range(blocks):
                if q != r:
                    remote(ld_rows(r, core), ld_rows(r, core), ld_sem, q, r, (leaf, q)).start()

    lanes = idx_ref.shape[2]

    def hits(first, count, level):
        wanted = first + lax.broadcasted_iota(jnp.int32, (count, lanes), 0)
        return jnp.where(wanted == idx_ref[0, level : level + 1, :], 1.0, 0.0).astype(BF16)

    def placed(marks, both):
        return lax.dot_general(
            marks, both, (((1,), (0,)), ((), ())), preferred_element_type=F32
        )

    loads[4].wait()
    both0 = jnp.concatenate(split(front[0]), axis=1)

    def place_step(q, carry):
        for slot, anc in enumerate((2, 0, 1)):
            rows = placed(hits(anc * sep + q * width, width, 0), both0).astype(BF16)
            for k in range(2):
                piece = rows[:, k * width : (k + 1) * width]
                if slot == 0:
                    place_t[k, q] = piece
                else:
                    place_u[k, q, (slot - 1) * width : slot * width, :] = piece
        return carry

    lax.fori_loop(0, blocks, place_step, 0)
    loads[5].wait()

    def g_copy(q):
        return remote(spread.at[q], gather_f.at[me, core], g_sem, q, me, (leaf, q))

    def g_arrival(r):
        return remote(gather_f.at[r, core], gather_f.at[r, core], g_sem, r, r, (leaf, r))

    def spread_front():
        both1 = jnp.concatenate(split(front[1]), axis=1)

        def step(q, carry):
            rows = placed(hits(core * sep + q * width, width, 1), both1)
            spread[q] = rows[:, :width] + rows[:, width:]
            return carry

        lax.fori_loop(0, blocks, step, 0)
        gather_f[me, core] = spread[me]
        for q in range(blocks):
            @pl.when(q != me)
            def _():
                g_copy(q).start()

    late = blocks // 2

    @pl.when(me >= late)
    def _():
        spread_front()

    @pl.when(me >= 1)
    def _():
        sol_ref[0, 0] = rs_ref[0, 0]
        for e in range(blocks - 1):
            @pl.when(e < me)
            def _():
                right = split(ld0[:, (e + 1) * width : (e + 2) * width])
                x_arrival(e).wait_recv()
                sol_ref[0, 0] = sol_ref[0, 0] - product(split(xs[e]), right)
        finish_x(sol_ref[0, 0])

    x_own = xs[me]
    sol_ref[0, 0] = x_own
    x_parts = split(x_own)

    def piece_copy(parts, lands, sems, q, c):
        return remote(
            parts.at[q, c],
            lands.at[2 * me + core],
            sems,
            2 * q + c,
            2 * me + core,
            (first_leaf + c, q),
        )

    def is_other(q, c):
        return (q != me) | (c != core)

    def send_pieces(parts, lands, sems):
        for q in range(blocks):
            for c in range(2):
                @pl.when(is_other(q, c))
                def _():
                    piece_copy(parts, lands, sems, q, c).start()

    for q in range(blocks):
        update = product(x_parts, (place_t[0, q], place_t[1, q]))
        for c in range(2):
            part_t[q, c] = update[c * half : (c + 1) * half]
    send_pieces(part_t, recv_t, t_sem)
    for q in range(blocks):
        update = product(x_parts, (place_u[0, q], place_u[1, q]))
        for c in range(2):
            part_u[q, c] = update[c * half : (c + 1) * half]

    @pl.when(me < blocks - 1)
    def _():
        send_pieces(part_u, recv_u, u_sem)

    @pl.when(me < late)
    def _():
        spread_front()

    def ld_forward(r):
        return remote(ld_rows(r, core), ld_rows(r, core), lf_sem, r, r, partner)

    def ld_forward_in(r):
        return remote(ld_rows(r, 1 - core), ld_rows(r, 1 - core), lf_sem, r, r, partner)

    def g_forward(r):
        return remote(gather_f.at[r, core], gather_f.at[r, core], gf_sem, r, r, partner)

    def g_forward_in(r):
        return remote(gather_f.at[r, 1 - core], gather_f.at[r, 1 - core], gf_sem, r, r, partner)

    for r in range(blocks):
        @pl.when(r != me)
        def _():
            remote(ld_rows(r, core), ld_rows(r, core), ld_sem, r, r, (leaf, r)).wait_recv()
            ld_forward(r).start()
            g_arrival(r).wait_recv()
        g_forward(r).start()

    def piece_arrival(parts, lands, sems, r, c):
        return remote(parts.at[r, c], lands.at[2 * r + c], sems, 2 * r + c, 2 * r + c, (first_leaf + c, r))

    recv_t[2 * me + core] = part_t[me, core]
    total = None
    for r in range(blocks):
        for c in range(2):
            @pl.when(is_other(r, c))
            def _():
                piece_arrival(part_t, recv_t, t_sem, r, c).wait_recv()
    total = recv_t[0]
    for s in range(1, 2 * blocks):
        total = total + recv_t[s]
    first_row = pl.multiple_of(core * half, half)
    ag[me] = rs_ref[0, 1, pl.ds(first_row, half), :] - total

    def ag_copy(q):
        return remote(ag.at[me], ag.at[me], ag_sem, q, me, (leaf, q))

    for q in range(blocks):
        @pl.when(q != me)
        def _():
            ag_copy(q).start()

    @pl.when(me == blocks - 1)
    def _():
        send_pieces(part_u, recv_u, u_sem)

    for r in range(blocks):
        @pl.when(r != me)
        def _():
            ld_forward_in(r).wait_recv()
        g_forward_in(r).wait_recv()

    solved = []
    top = None
    for b in range(blocks):
        @pl.when(b != me)
        def _():
            remote(ag.at[b], ag.at[b], ag_sem, b, b, (leaf, b)).wait_recv()
        total = ag[b]
        if b > 1:
            older = [jnp.concatenate([x[k] for x in solved[:-1]], axis=1) for k in range(2)]
            total = total - product(older, split(ld1[b, :, width : b * width]))
        if b > 0:
            total = total - product(solved[-1], split(ld1[b, :, b * width : (b + 1) * width]))
        x = product(split(total), split(ld1[b, :, :width]))

        @pl.when(b == me)
        def _():
            own_half[0] = x

        solved.append(split(x))
        added = [
            product(solved[-1], split(gather_f[b, k])) for k in range(2)
        ]
        top = added if top is None else [top[k] + added[k] for k in range(2)]

    def half_copy(k):
        return remote(own_half.at[k], other_half.at[k], out_sem, k, k, partner)

    recv_u[2 * me + core] = part_u[me, core]
    for r in range(blocks):
        for c in range(2):
            @pl.when(is_other(r, c))
            def _():
                piece_arrival(part_u, recv_u, u_sem, r, c).wait_recv()
    slot0 = recv_u[0]
    for s in range(1, 2 * blocks):
        slot0 = slot0 + recv_u[s]
    for k in range(2):
        own_half[1 + k] = top[k] + slot0[:, k * width : (k + 1) * width]
    for k in range(3):
        half_copy(k).start()
    other_row = pl.multiple_of((1 - core) * half, half)
    sol_ref[0, 1, pl.ds(first_row, half), :] = own_half[0]
    for k in range(2):
        top_ref[0, k, pl.ds(first_row, half), :] = own_half[1 + k]

    for q in range(blocks):
        @pl.when(q > me)
        def _():
            x_copy(q).wait_send()
        @pl.when(q != me)
        def _():
            ag_copy(q).wait_send()
            g_copy(q).wait_send()
            ld_forward(q).wait_send()
        g_forward(q).wait_send()
        for c in range(2):
            @pl.when(is_other(q, c))
            def _():
                piece_copy(part_t, recv_t, t_sem, q, c).wait_send()
                piece_copy(part_u, recv_u, u_sem, q, c).wait_send()
    for r in range(blocks):
        @pl.when(me == r)
        def _():
            for q in range(blocks):
                if q != r:
                    remote(ld_rows(r, core), ld_rows(r, core), ld_sem, q, r, (leaf, q)).wait_send()

    for k in range(3):
        half_copy(k).wait()
    sol_ref[0, 1, pl.ds(other_row, half), :] = other_half[0]
    for k in range(2):
        top_ref[0, k, pl.ds(other_row, half), :] = other_half[1 + k]


def on_device(right_side, diag_inverse, sep_lower, front_lower, front_index):
    blocks = lax.axis_size("rows")
    vectors, width = right_side.shape[2:]
    reach = front_lower.shape[2]
    half = vectors // 2
    sep = blocks * width
    vmem = pl.BlockSpec(memory_space=pltpu.VMEM)
    hbm = pl.BlockSpec(memory_space=pl.ANY)
    dma = pltpu.SemaphoreType.DMA
    return pl.pallas_call(
        functools.partial(kernel, blocks),
        out_shape=(
            jax.ShapeDtypeStruct((1, 2, vectors, width), F32),
            jax.ShapeDtypeStruct((1, 2, vectors, width), F32),
        ),
        in_specs=[vmem, vmem, hbm, hbm, hbm],
        out_specs=(vmem, vmem),
        scratch_shapes=[
            pltpu.VMEM((width, sep + width), F32),
            pltpu.VMEM((blocks, width, sep + width), F32),
            pltpu.VMEM((2, reach, width), F32),
            pltpu.VMEM((2, blocks, width, width), BF16),
            pltpu.VMEM((2, blocks, 2 * width, width), BF16),
            pltpu.VMEM((blocks, width, width), F32),
            pltpu.VMEM((blocks, 2, width, width), F32),
            pltpu.VMEM((blocks, vectors, width), F32),
            pltpu.VMEM((blocks, 2, half, width), F32),
            pltpu.VMEM((blocks, 2, half, 2 * width), F32),
            pltpu.VMEM((2 * blocks, half, width), F32),
            pltpu.VMEM((2 * blocks, half, 2 * width), F32),
            pltpu.VMEM((blocks, half, width), F32),
            pltpu.VMEM((3, half, width), F32),
            pltpu.VMEM((3, half, width), F32),
            dma((6,)),
            dma((2, blocks)),
            dma((2, blocks)),
            dma((2, blocks)),
            dma((2, blocks)),
            dma((2, blocks)),
            dma((2, 2 * blocks)),
            dma((2, 2 * blocks)),
            dma((2, blocks)),
            dma((2, 3)),
        ],
        compiler_params=pltpu.CompilerParams(
            collective_id=0, has_side_effects=True, vmem_limit_bytes=60 * 1024 * 1024
        ),
    )(right_side, front_index, diag_inverse, sep_lower, front_lower)


def solution(mesh):
    in_specs = (
        P("leaf", None, None, "rows"),
        P("leaf", None, "rows", None),
        P("leaf", None, "rows", None),
        P("leaf", None, None, "rows"),
        P("leaf", None, None),
    )
    out_specs = (P("leaf", None, None, "rows"), P("leaf", None, None, "rows"))
    return jax.shard_map(
        on_device, mesh=mesh, in_specs=in_specs, out_specs=out_specs, check_vma=False
    )
```

```python
import functools

import jax
import jax.numpy as jnp
from jax import lax
from jax.experimental import pallas as pl
from jax.experimental.pallas import tpu as pltpu
from jax.sharding import PartitionSpec as P

MESH = pl.DeviceIdType.MESH
F32 = jnp.float32
BF16 = jnp.bfloat16


def split(value):
    high = value.astype(BF16)
    low = (value - high.astype(F32)).astype(BF16)
    return high, low


def dot_nt(left, right):
    return lax.dot_general(
        left, right, (((1,), (1,)), ((), ())), preferred_element_type=F32
    )


def product(left, right):
    return (
        dot_nt(left[0], right[1]) + dot_nt(left[1], right[0])
    ) + dot_nt(left[0], right[0])


def kernel(
    blocks,
    rs_ref,
    idx_ref,
    diag_hbm,
    lower_hbm,
    front_hbm,
    sol_ref,
    top_ref,
    factor,
    front,
    weight,
    place_t,
    place_u,
    place_v,
    total,
    xs0,
    xs1,
    part_t,
    recv_t,
    part_u,
    recv_u,
    part_v,
    recv_v,
    top_half,
    top_other,
    x_other,
    load_sem,
    x0_sem,
    x1_sem,
    t_sem,
    v_sem,
    pair_sem,
):
    vectors, width = rs_ref.shape[2], rs_ref.shape[3]
    half = vectors // 2
    sep = blocks * width
    lanes = idx_ref.shape[2]
    leaf = lax.axis_index("leaf")
    me = lax.axis_index("rows")
    core = lax.rem(leaf, 2)
    first_leaf = leaf - core
    partner = (leaf + 1 - 2 * core, me)
    first_row = pl.multiple_of(core * half, half)
    other_row = pl.multiple_of((1 - core) * half, half)

    def remote(src, dst, sems, out_slot, in_slot, device):
        return pltpu.make_async_remote_copy(
            src_ref=src,
            dst_ref=dst,
            send_sem=sems.at[0, out_slot],
            recv_sem=sems.at[1, in_slot],
            device_id=device,
            device_id_type=MESH,
        )

    barrier = pltpu.get_barrier_semaphore()
    pl.semaphore_signal(barrier, inc=1, device_id=partner, device_id_type=MESH)
    for q in range(blocks):
        @pl.when(q != me)
        def _():
            for c in range(2):
                pl.semaphore_signal(
                    barrier, inc=1, device_id=(first_leaf + c, q), device_id_type=MESH
                )

    loads = []
    for level in range(2):
        for src, dst in (
            (diag_hbm.at[0, level], factor.at[level, :, pl.ds(0, width)]),
            (lower_hbm.at[0, level], factor.at[level, :, pl.ds(width, sep)]),
            (front_hbm.at[0, level], front.at[level]),
        ):
            loads.append(pltpu.make_async_copy(src, dst, load_sem.at[len(loads)]))
    for load in loads:
        load.start()

    def split_factor(level):
        loads[3 * level].wait()
        loads[3 * level + 1].wait()
        for k, piece in enumerate(split(factor[level])):
            weight[level, k] = piece

    def weights(level, b):
        return tuple(weight[level, k, :, b * width : (b + 1) * width] for k in range(2))

    split_factor(0)

    @pl.when(me == 0)
    def _():
        xs0[me] = product(split(rs_ref[0, 0]), weights(0, 0))

    def hits(first, level):
        wanted = first + lax.broadcasted_iota(jnp.int32, (width, lanes), 0)
        return jnp.where(wanted == idx_ref[0, level : level + 1, :], 1.0, 0.0).astype(BF16)

    def placed(marks, both):
        return lax.dot_general(
            marks, both, (((1,), (0,)), ((), ())), preferred_element_type=F32
        ).astype(BF16)

    loads[2].wait()
    both0 = jnp.concatenate(split(front[0]), axis=1)

    def place_step0(q, carry):
        for slot, anc in enumerate((2, 0, 1)):
            rows = placed(hits(anc * sep + q * width, 0), both0)
            for k in range(2):
                piece = rows[:, k * width : (k + 1) * width]
                if slot == 0:
                    place_t[k, q] = piece
                else:
                    place_u[k, q, (slot - 1) * width : slot * width, :] = piece
        return carry

    lax.fori_loop(0, blocks, place_step0, 0)
    split_factor(1)
    loads[5].wait()
    both1 = jnp.concatenate(split(front[1]), axis=1)

    def place_step1(q, carry):
        for slot in range(2):
            rows = placed(hits(slot * sep + q * width, 1), both1)
            for k in range(2):
                piece = rows[:, k * width : (k + 1) * width]
                place_v[k, q, slot * width : (slot + 1) * width, :] = piece
        return carry

    lax.fori_loop(0, blocks, place_step1, 0)

    pl.semaphore_wait(barrier, 2 * blocks - 1)

    def x_copy(xs, sems, q):
        return remote(xs.at[me], xs.at[me], sems, q, me, (leaf, q))

    def send_x(xs, sems):
        for q in range(1, blocks):
            @pl.when(q > me)
            def _():
                x_copy(xs, sems, q).start()

    def subtract_solved(level, xs, sems, rows):
        for e in range(blocks - 1):
            @pl.when(e < me)
            def _():
                right = weights(level, e + 1)
                remote(xs.at[e], xs.at[e], sems, e, e, (leaf, e)).wait_recv()
                total[:rows] = total[:rows] - product(split(xs[e]), right)

    @pl.when(me >= 1)
    def _():
        total[...] = rs_ref[0, 0]
        subtract_solved(0, xs0, x0_sem, vectors)
        xs0[me] = product(split(total[...]), weights(0, 0))

    send_x(xs0, x0_sem)
    x_parts = split(xs0[me])

    def is_other(q, c):
        return (q != me) | (c != core)

    def t_copy(q, c):
        return remote(
            part_t.at[q, c],
            recv_t.at[2 * me + core],
            t_sem,
            2 * q + c,
            2 * me + core,
            (first_leaf + c, q),
        )

    for q in range(blocks):
        update = product(x_parts, (place_t[0, q], place_t[1, q]))
        for c in range(2):
            part_t[q, c] = update[c * half : (c + 1) * half]
        for c in range(2):
            @pl.when(is_other(q, c))
            def _():
                t_copy(q, c).start()
    sol_ref[0, 0] = xs0[me]
    for q in range(blocks):
        update = product(x_parts, (place_u[0, q], place_u[1, q]))
        for c in range(2):
            part_u[c, q] = update[c * half : (c + 1) * half]

    u_copy = remote(part_u.at[1 - core], recv_u, pair_sem, 0, 0, partner)
    u_copy.start()
    total[:half] = rs_ref[0, 1, pl.ds(first_row, half), :] - part_t[me, core]
    u_copy.wait_recv()
    for q in range(blocks):
        part_v[q] = part_u[core, q] + recv_u[q]
    for r in range(blocks):
        for c in range(2):
            @pl.when(is_other(r, c))
            def _():
                s = 2 * r + c
                remote(part_t.at[r, c], recv_t.at[s], t_sem, s, s, (first_leaf + c, r)).wait_recv()
                total[:half] = total[:half] - recv_t[s]

    subtract_solved(1, xs1, x1_sem, half)
    xs1[me] = product(split(total[:half]), weights(1, 0))
    send_x(xs1, x1_sem)
    x_out = remote(xs1.at[me], x_other, pair_sem, 1, 1, partner)
    x_parts = split(xs1[me])

    def v_copy(q):
        return remote(part_v.at[q], recv_v.at[me], v_sem, q, me, (leaf, q))

    for q in range(blocks):
        part_v[q] = part_v[q] + product(x_parts, (place_v[0, q], place_v[1, q]))

        @pl.when(q != me)
        def _():
            v_copy(q).start()

    x_out.start()
    sol_ref[0, 1, pl.ds(first_row, half), :] = xs1[me]
    top_half[...] = part_v[me]
    for r in range(blocks):
        @pl.when(r != me)
        def _():
            remote(part_v.at[r], recv_v.at[r], v_sem, r, r, (leaf, r)).wait_recv()
            top_half[...] = top_half[...] + recv_v[r]
    top_out = remote(top_half, top_other, pair_sem, 2, 2, partner)
    top_out.start()
    for k in range(2):
        top_ref[0, k, pl.ds(first_row, half), :] = top_half[:, k * width : (k + 1) * width]
    u_copy.wait_send()
    for q in range(blocks):
        @pl.when(q > me)
        def _():
            x_copy(xs0, x0_sem, q).wait_send()
            x_copy(xs1, x1_sem, q).wait_send()
        @pl.when(q != me)
        def _():
            v_copy(q).wait_send()
        for c in range(2):
            @pl.when(is_other(q, c))
            def _():
                t_copy(q, c).wait_send()
    x_out.wait()
    sol_ref[0, 1, pl.ds(other_row, half), :] = x_other[...]
    top_out.wait()
    for k in range(2):
        top_ref[0, k, pl.ds(other_row, half), :] = top_other[:, k * width : (k + 1) * width]


def on_device(right_side, diag_inverse, sep_lower, front_lower, front_index):
    blocks = lax.axis_size("rows")
    vectors, width = right_side.shape[2:]
    reach = front_lower.shape[2]
    half = vectors // 2
    sep = blocks * width
    vmem = pl.BlockSpec(memory_space=pltpu.VMEM)
    hbm = pl.BlockSpec(memory_space=pl.ANY)
    dma = pltpu.SemaphoreType.DMA
    return pl.pallas_call(
        functools.partial(kernel, blocks),
        out_shape=(
            pltpu.VMEM((1, 2, vectors, width), F32),
            pltpu.VMEM((1, 2, vectors, width), F32),
        ),
        in_specs=[vmem, vmem, hbm, hbm, hbm],
        out_specs=(vmem, vmem),
        scratch_shapes=[
            pltpu.VMEM((2, width, sep + width), F32),
            pltpu.VMEM((2, reach, width), F32),
            pltpu.VMEM((2, 2, width, sep + width), BF16),
            pltpu.VMEM((2, blocks, width, width), BF16),
            pltpu.VMEM((2, blocks, 2 * width, width), BF16),
            pltpu.VMEM((2, blocks, 2 * width, width), BF16),
            pltpu.VMEM((vectors, width), F32),
            pltpu.VMEM((blocks, vectors, width), F32),
            pltpu.VMEM((blocks, half, width), F32),
            pltpu.VMEM((blocks, 2, half, width), F32),
            pltpu.VMEM((2 * blocks, half, width), F32),
            pltpu.VMEM((2, blocks, half, 2 * width), F32),
            pltpu.VMEM((blocks, half, 2 * width), F32),
            pltpu.VMEM((blocks, half, 2 * width), F32),
            pltpu.VMEM((blocks, half, 2 * width), F32),
            pltpu.VMEM((half, 2 * width), F32),
            pltpu.VMEM((half, 2 * width), F32),
            pltpu.VMEM((half, width), F32),
            dma((6,)),
            dma((2, blocks)),
            dma((2, blocks)),
            dma((2, 2 * blocks)),
            dma((2, blocks)),
            dma((2, 3)),
        ],
        compiler_params=pltpu.CompilerParams(
            collective_id=0, has_side_effects=True, vmem_limit_bytes=60 * 1024 * 1024
        ),
    )(right_side, front_index, diag_inverse, sep_lower, front_lower)


def solution(mesh):
    in_specs = (
        P("leaf", None, None, "rows"),
        P("leaf", None, "rows", None),
        P("leaf", None, "rows", None),
        P("leaf", None, None, "rows"),
        P("leaf", None, None),
    )
    out_specs = (P("leaf", None, None, "rows"), P("leaf", None, None, "rows"))
    return jax.shard_map(
        on_device, mesh=mesh, in_specs=in_specs, out_specs=out_specs, check_vma=False
    )
```

```python
import functools

import jax
import jax.numpy as jnp
from jax import lax
from jax.experimental import pallas as pl
from jax.experimental.pallas import tpu as pltpu
from jax.sharding import PartitionSpec as P

MESH = pl.DeviceIdType.MESH
F32 = jnp.float32
BF16 = jnp.bfloat16


def split(value):
    high = value.astype(BF16)
    low = (value - high.astype(F32)).astype(BF16)
    return high, low


def dot_nt(left, right):
    return lax.dot_general(
        left, right, (((1,), (1,)), ((), ())), preferred_element_type=F32
    )


def product(left, right):
    return (
        dot_nt(left[0], right[1]) + dot_nt(left[1], right[0])
    ) + dot_nt(left[0], right[0])


def kernel(
    blocks,
    rs_ref,
    idx_ref,
    diag_hbm,
    lower_hbm,
    front_hbm,
    sol_ref,
    top_ref,
    factor,
    rows1,
    front,
    weight,
    place_t,
    place_u,
    place_v,
    total,
    xs0,
    xs1,
    part_t,
    recv_t,
    part_u,
    recv_u,
    part_v,
    recv_v,
    top_half,
    top_other,
    x_other,
    load_sem,
    ld_sem,
    lf_sem,
    x0_sem,
    x1_sem,
    t_sem,
    v_sem,
    pair_sem,
):
    vectors, width = rs_ref.shape[2], rs_ref.shape[3]
    half = vectors // 2
    sep = blocks * width
    lanes = idx_ref.shape[2]
    leaf = lax.axis_index("leaf")
    me = lax.axis_index("rows")
    core = lax.rem(leaf, 2)
    first_leaf = leaf - core
    partner = (leaf + 1 - 2 * core, me)
    first_row = pl.multiple_of(core * half, half)
    other_row = pl.multiple_of((1 - core) * half, half)

    def remote(src, dst, sems, out_slot, in_slot, device):
        return pltpu.make_async_remote_copy(
            src_ref=src,
            dst_ref=dst,
            send_sem=sems.at[0, out_slot],
            recv_sem=sems.at[1, in_slot],
            device_id=device,
            device_id_type=MESH,
        )

    barrier = pltpu.get_barrier_semaphore()
    pl.semaphore_signal(barrier, inc=1, device_id=partner, device_id_type=MESH)
    for q in range(blocks):
        @pl.when(q != me)
        def _():
            for c in range(2):
                pl.semaphore_signal(
                    barrier, inc=1, device_id=(first_leaf + c, q), device_id_type=MESH
                )

    center = blocks // 2
    groups = min(blocks, 4)
    per = blocks // groups
    loads = []
    for level, held in enumerate((factor, rows1.at[me])):
        for src, dst in (
            (diag_hbm.at[0, level], held.at[:, pl.ds(0, width)]),
            (lower_hbm.at[0, level], held.at[:, pl.ds(width, sep)]),
            (front_hbm.at[0, level], front.at[level]),
        ):
            loads.append(pltpu.make_async_copy(src, dst, load_sem.at[len(loads)]))
    for load in loads:
        load.start()

    loads[0].wait()
    loads[1].wait()
    for k, piece in enumerate(split(factor[...])):
        weight[k] = piece

    def weights(b):
        return tuple(weight[k, :, b * width : (b + 1) * width] for k in range(2))

    @pl.when(me == 0)
    def _():
        xs0[me] = product(split(rs_ref[0, 0]), weights(0))

    def hits(first, level):
        wanted = first + lax.broadcasted_iota(jnp.int32, (width, lanes), 0)
        return jnp.where(wanted == idx_ref[0, level : level + 1, :], 1.0, 0.0).astype(BF16)

    def placed(marks, both):
        return lax.dot_general(
            marks, both, (((1,), (0,)), ((), ())), preferred_element_type=F32
        ).astype(BF16)

    loads[2].wait()
    both0 = jnp.concatenate(split(front[0]), axis=1)

    def place_step0(q, carry):
        for slot, anc in enumerate((2, 0, 1)):
            rows = placed(hits(anc * sep + q * width, 0), both0)
            for k in range(2):
                piece = rows[:, k * width : (k + 1) * width]
                if slot == 0:
                    place_t[k, q] = piece
                else:
                    place_u[k, q, (slot - 1) * width : slot * width, :] = piece
        return carry

    lax.fori_loop(0, blocks, place_step0, 0)
    loads[3].wait()
    loads[4].wait()
    loads[5].wait()
    both1 = jnp.concatenate(split(front[1]), axis=1)

    def place_step1(q, carry):
        for slot in range(2):
            rows = placed(hits(slot * sep + q * width, 1), both1)
            for k in range(2):
                piece = rows[:, k * width : (k + 1) * width]
                place_v[k, q, slot * width : (slot + 1) * width, :] = piece
        return carry

    lax.fori_loop(0, blocks, place_step1, 0)

    pl.semaphore_wait(barrier, 2 * blocks - 1)

    def x_copy(q):
        return remote(xs0.at[me], xs0.at[me], x0_sem, q, me, (leaf, q))

    def send_x():
        for q in range(1, blocks):
            @pl.when(q > me)
            def _():
                x_copy(q).start()

    def half_rows(r, c):
        return rows1.at[
            r,
            pl.ds(pl.multiple_of(c * (width // 2), width // 2), width // 2),
            pl.ds(0, (r + 1) * width),
        ]

    def row_copy(r):
        part = half_rows(r, core)
        return remote(part, part, ld_sem, r, r, (leaf, center))

    def row_forward(r, c):
        part = half_rows(r, c)
        return remote(part, part, lf_sem, r, r, partner)

    outer = [r for r in range(blocks) if r != center]

    @pl.when(me == 0)
    def _():
        send_x()

    for r in outer:
        @pl.when(me == r)
        def _():
            row_copy(r).start()

    @pl.when(me >= 1)
    def _():
        total[...] = rs_ref[0, 0]
        for e in range(blocks - 1):
            @pl.when(e < me)
            def _():
                right = weights(e + 1)
                remote(xs0.at[e], xs0.at[e], x0_sem, e, e, (leaf, e)).wait_recv()
                total[...] = total[...] - product(split(xs0[e]), right)
        xs0[me] = product(split(total[...]), weights(0))
        send_x()

    x_parts = split(xs0[me])

    def is_other(r, c):
        return (r != me) | (c != core)

    def t_copy(g, c):
        span = pl.ds(g * per, per)
        return remote(
            part_t.at[c, span],
            recv_t.at[2 * me + core, span],
            t_sem,
            groups * c + g,
            groups * (2 * me + core) + g,
            (first_leaf + c, center),
        )

    def t_arrival(r, c, g):
        span = pl.ds(g * per, per)
        s = 2 * r + c
        return pltpu.make_async_remote_copy(
            src_ref=part_t.at[c, span],
            dst_ref=recv_t.at[s, span],
            send_sem=t_sem.at[0, g],
            recv_sem=t_sem.at[1, groups * s + g],
            device_id=(first_leaf + c, r),
            device_id_type=MESH,
        )

    for q in range(blocks):
        update = product(x_parts, (place_t[0, q], place_t[1, q]))
        update = update - jnp.where((me == q) & (core == 0), rs_ref[0, 1], 0.0)
        for c in range(2):
            part_t[c, q] = update[c * half : (c + 1) * half]
        if (q + 1) % per == 0:
            for c in range(2):
                @pl.when((me != center) | (c != core))
                def _():
                    t_copy(q // per, c).start()
    sol_ref[0, 0] = xs0[me]
    for q in range(blocks):
        update = product(x_parts, (place_u[0, q], place_u[1, q]))
        for c in range(2):
            part_u[c, q] = update[c * half : (c + 1) * half]

    u_copy = remote(part_u.at[1 - core], recv_u, pair_sem, 0, 0, partner)
    u_copy.start()
    u_copy.wait_recv()
    for q in range(blocks):
        part_v[q] = part_u[core, q] + recv_u[q]

    def x1_copy(b):
        return remote(xs1.at[b], xs1.at[b], x1_sem, b, b, (leaf, b))

    @pl.when(me == center)
    def _():
        for r in outer:
            row_copy(r).wait_recv()
            row_forward(r, core).start()
        recv_t[2 * center + core] = part_t[core]
        for r in outer:
            row_forward(r, 1 - core).wait_recv()
        solved = []
        for b in range(blocks):
            if b % per == 0:
                for r in range(blocks):
                    for c in range(2):
                        @pl.when(is_other(r, c))
                        def _():
                            t_arrival(r, c, b // per).wait_recv()
            value = -recv_t[0, b]
            for s in range(1, 2 * blocks):
                value = value - recv_t[s, b]
            if b > 1:
                older = [jnp.concatenate([x[k] for x in solved[:-1]], axis=1) for k in range(2)]
                value = value - product(older, split(rows1[b, :, width : b * width]))
            if b > 0:
                value = value - product(
                    solved[-1], split(rows1[b, :, b * width : (b + 1) * width])
                )
            x = product(split(value), split(rows1[b, :, :width]))
            xs1[b] = x
            if b != center:
                x1_copy(b).start()
            solved.append(split(x))
        for r in outer:
            row_forward(r, core).wait_send()
            x1_copy(r).wait_send()

    for r in outer:
        @pl.when(me == r)
        def _():
            x1_copy(r).wait_recv()

    x_out = remote(xs1.at[me], x_other, pair_sem, 1, 1, partner)
    x_parts = split(xs1[me])

    def v_copy(q):
        return remote(part_v.at[q], recv_v.at[me], v_sem, q, me, (leaf, q))

    for q in range(blocks):
        part_v[q] = part_v[q] + product(x_parts, (place_v[0, q], place_v[1, q]))

        @pl.when(q != me)
        def _():
            v_copy(q).start()

    x_out.start()
    sol_ref[0, 1, pl.ds(first_row, half), :] = xs1[me]
    top_half[...] = part_v[me]
    for r in range(blocks):
        @pl.when(r != me)
        def _():
            remote(part_v.at[r], recv_v.at[r], v_sem, r, r, (leaf, r)).wait_recv()
            top_half[...] = top_half[...] + recv_v[r]
    top_out = remote(top_half, top_other, pair_sem, 2, 2, partner)
    top_out.start()
    for k in range(2):
        top_ref[0, k, pl.ds(first_row, half), :] = top_half[:, k * width : (k + 1) * width]
    u_copy.wait_send()
    for c in range(2):
        @pl.when((me != center) | (c != core))
        def _():
            for g in range(groups):
                t_copy(g, c).wait_send()
    for r in outer:
        @pl.when(me == r)
        def _():
            row_copy(r).wait_send()
    for q in range(blocks):
        @pl.when(q > me)
        def _():
            x_copy(q).wait_send()
        @pl.when(q != me)
        def _():
            v_copy(q).wait_send()
    x_out.wait()
    sol_ref[0, 1, pl.ds(other_row, half), :] = x_other[...]
    top_out.wait()
    for k in range(2):
        top_ref[0, k, pl.ds(other_row, half), :] = top_other[:, k * width : (k + 1) * width]


def on_device(right_side, diag_inverse, sep_lower, front_lower, front_index):
    blocks = lax.axis_size("rows")
    vectors, width = right_side.shape[2:]
    reach = front_lower.shape[2]
    half = vectors // 2
    sep = blocks * width
    vmem = pl.BlockSpec(memory_space=pltpu.VMEM)
    hbm = pl.BlockSpec(memory_space=pl.ANY)
    dma = pltpu.SemaphoreType.DMA
    return pl.pallas_call(
        functools.partial(kernel, blocks),
        out_shape=(
            pltpu.VMEM((1, 2, vectors, width), F32),
            pltpu.VMEM((1, 2, vectors, width), F32),
        ),
        in_specs=[vmem, vmem, hbm, hbm, hbm],
        out_specs=(vmem, vmem),
        scratch_shapes=[
            pltpu.VMEM((width, sep + width), F32),
            pltpu.VMEM((blocks, width, sep + width), F32),
            pltpu.VMEM((2, reach, width), F32),
            pltpu.VMEM((2, width, sep + width), BF16),
            pltpu.VMEM((2, blocks, width, width), BF16),
            pltpu.VMEM((2, blocks, 2 * width, width), BF16),
            pltpu.VMEM((2, blocks, 2 * width, width), BF16),
            pltpu.VMEM((vectors, width), F32),
            pltpu.VMEM((blocks, vectors, width), F32),
            pltpu.VMEM((blocks, half, width), F32),
            pltpu.VMEM((2, blocks, half, width), F32),
            pltpu.VMEM((2 * blocks, blocks, half, width), F32),
            pltpu.VMEM((2, blocks, half, 2 * width), F32),
            pltpu.VMEM((blocks, half, 2 * width), F32),
            pltpu.VMEM((blocks, half, 2 * width), F32),
            pltpu.VMEM((blocks, half, 2 * width), F32),
            pltpu.VMEM((half, 2 * width), F32),
            pltpu.VMEM((half, 2 * width), F32),
            pltpu.VMEM((half, width), F32),
            dma((6,)),
            dma((2, blocks)),
            dma((2, blocks)),
            dma((2, blocks)),
            dma((2, blocks)),
            dma((2, 2 * blocks * min(blocks, 4))),
            dma((2, blocks)),
            dma((2, 3)),
        ],
        compiler_params=pltpu.CompilerParams(
            collective_id=0, has_side_effects=True, vmem_limit_bytes=60 * 1024 * 1024
        ),
    )(right_side, front_index, diag_inverse, sep_lower, front_lower)


def solution(mesh):
    in_specs = (
        P("leaf", None, None, "rows"),
        P("leaf", None, "rows", None),
        P("leaf", None, "rows", None),
        P("leaf", None, None, "rows"),
        P("leaf", None, None),
    )
    out_specs = (P("leaf", None, None, "rows"), P("leaf", None, None, "rows"))
    return jax.shard_map(
        on_device, mesh=mesh, in_specs=in_specs, out_specs=out_specs, check_vma=False
    )
```
